32 devices in a mesh: grp: 2 (over y), seq: 4 (over z), dp: 2 (over x), tp: 2 (over core).
Axes of the slice: x: 2, y: 2, z: 4, core: 2. Of those that a mesh axis runs over, the one named last changes fastest.
Arguments:
- query_image: bfloat16 [4, 1024, 2048], P(('grp', 'dp'), ('seq', 'tp')), parts along dimension 0, may hold values from -8 to 8
- key_image: bfloat16 [4, 1024, 2048], P(('grp', 'dp'), ('seq', 'tp')), parts along dimension 0, may hold values from -8 to 8
- value_image: bfloat16 [4, 1024, 2048], P(('grp', 'dp'), ('seq', 'tp')), parts along dimension 0, may hold values from -6 to 6
- query_text: bfloat16 [4, 128, 2048], P(('grp', 'dp'), ('seq', 'tp')), parts along dimension 0, may hold values from -6 to 6
- key_text: bfloat16 [4, 128, 2048], P(('grp', 'dp'), ('seq', 'tp')), parts along dimension 0, may hold values from -6 to 6
- value_text: bfloat16 [4, 128, 2048], P(('grp', 'dp'), ('seq', 'tp')), parts along dimension 0, may hold values from -6 to 6
- image_query_gain: float32 [128], replicated, may hold values from 1 to 6
- image_key_gain: float32 [128], replicated, may hold values from 1 to 6
- text_query_gain: float32 [128], replicated, may hold values from 1.2 to 2.5
- text_key_gain: float32 [128], replicated, may hold values from 1.2 to 2.5
- text_length: int32 [4], P(('grp', 'dp')), parts along dimension 0, may hold values from 1 to 128
- strata: int32 [4], P(('grp', 'dp')), parts along dimension 0, may hold values from 0 to 63
- image_state: bfloat16 [4, 1024, 3072], P(('grp', 'dp'), ('seq', 'tp')), parts along dimension 0, may hold values from -6 to 6
- target: bfloat16 [4, 1024, 3072], P(('grp', 'dp'), ('seq', 'tp')), parts along dimension 0, may hold values from -6 to 6
- out_weight: bfloat16 [2048, 3072], P('seq', 'tp'), may hold values from -0.125 to 0.125
- gate_table: bfloat16 [64, 3072], replicated, may hold values from -4 to 4
Outputs:
- velocity: bfloat16 [4, 1024, 3072], P(('grp', 'dp'), ('seq', 'tp')), parts along dimension 0
- text_attention: bfloat16 [4, 128, 2048], P(('grp', 'dp'), ('seq', 'tp')), parts along dimension 0
- flow_loss: float32 [2], P('grp'), parts along dimension 0
The draws below stay inside these ranges and needn't reach their ends.
There are 2 independent parts, one for each index of `grp`. The reference program is written for one: setup_inputs(seed, part) draws one part's arguments, and reference() takes and returns one part's arrays. A program takes and returns all parts, laid end to end along the dimension named above; an argument that names none is the same for every part. Nothing has to cross between parts.
Inputs may be any that keep to these rules, and one draw needn't show every extreme that they name: `text_length`: text positions at or beyond a sample's length are padding and are not attended to.
All inputs are finite; a program needn't handle non-finite values.
Results may differ from the reference program's by a relative error of at most 0.012.
The reference program's roundings to bfloat16 on the way count: a program that leaves them out, or rounds other values in their place, can miss the bound.
Values may be sent and summed in bfloat16 or wider, within the bound.
No kernel may reach another device: no remote copies, remote signals or barrier semaphores. Data moves between devices by JAX's collectives and lax.ppermute only.
A program may use at most 64 MiB of HBM per device.

```python
import math
import jax
import jax.numpy as jnp
from jax import lax

D = 3072
HEADS = 16
HEAD_DIM = 128
STRATA = 64
SAMPLES = 2
IMG = 1024
TXT = 128
ATTN = 2048


def drawn_pair(key):
    folded = jax.random.fold_in(key, 7331)
    draw_query, draw_key = jax.random.split(folded, 2)
    queries = jnp.clip(jax.random.normal(draw_query, (SAMPLES, IMG, HEADS * HEAD_DIM), jnp.float32), -6.0, 6.0)
    keys_drawn = jnp.clip(jax.random.normal(draw_key, (SAMPLES, IMG, HEADS * HEAD_DIM), jnp.float32), -6.0, 6.0)
    return (queries, keys_drawn)


def draw_query_image(key, part):
    return drawn_pair(key)[0].astype(jnp.bfloat16)


def draw_key_image(key, part):
    return drawn_pair(key)[1].astype(jnp.bfloat16)


def gain_draw(key):
    return jnp.exp(jax.random.uniform(key, (HEAD_DIM,), jnp.float32, jnp.log(1.2), jnp.log(2.5)))


def draw_image_query_gain(key, part):
    return gain_draw(jax.random.fold_in(key, 11))


def draw_image_key_gain(key, part):
    return gain_draw(jax.random.fold_in(key, 13))


def draw_target(key, part):
    folded = jax.random.fold_in(key, 29)
    draw_noise, draw_sample, draw_column = jax.random.split(folded, 3)
    rising = jnp.arange(IMG, dtype=jnp.float32) / IMG
    sample_offset = jax.random.uniform(draw_sample, (SAMPLES,), jnp.float32, -1.0, 1.0)
    column_offset = jnp.clip(0.5 * jax.random.normal(draw_column, (D,), jnp.float32), -1.0, 1.0)
    sample_noise = jnp.clip(jax.random.normal(draw_noise, (SAMPLES, IMG, D), jnp.float32), -2.5, 2.5)
    scaling = 0.5 + rising
    shared = sample_offset[:, None, None] + column_offset[None, None, :]
    return (sample_noise * scaling[None, :, None] + shared).astype(jnp.bfloat16)


def block_scale(own_key, extent, pieces, low, top_value):
    def one(dim, parts):
        draws = jax.random.uniform(jax.random.fold_in(jax.random.fold_in(own_key, 6), dim), (parts,), jnp.float32, low / len(pieces), top_value / len(pieces))
        return jnp.repeat(jnp.exp(draws), extent[dim] // parts).reshape((-1,) + (1,) * (len(extent) - dim - 1))

    gain = one(*pieces[0])
    for cut in pieces[1:]:
        gain = gain * one(*cut)
    return gain


def gaussian(own_key, dims, deviation, reach, pieces=(), kind=jnp.bfloat16):
    gain = block_scale(own_key, dims, pieces, -0.22, 0.18) if pieces else 1.0
    drawn = jax.random.normal(own_key, dims, jnp.float32) * deviation * gain
    return jnp.minimum(jnp.maximum(drawn, -reach), reach).astype(kind)


def setup_inputs(seed: int = 0, part: int = 0) -> dict:
    key_of = jax.random.split(jax.random.key(seed), 17)
    own_keys = jax.random.split(jax.random.fold_in(key_of[16], part), 17)
    query_image = draw_query_image(jax.random.fold_in(jax.random.fold_in(key_of[16], part), 71), part)
    key_image = draw_key_image(jax.random.fold_in(jax.random.fold_in(key_of[16], part), 71), part)
    value_image = gaussian(own_keys[2], (SAMPLES, IMG, ATTN), 1.0, 6.0, ((0, 2), (1, 8)))
    query_text = gaussian(own_keys[3], (SAMPLES, TXT, ATTN), 1.0, 6.0, ((0, 2), (1, 8)))
    key_text = gaussian(own_keys[4], (SAMPLES, TXT, ATTN), 1.0, 6.0, ((0, 2), (1, 8)))
    value_text = gaussian(own_keys[5], (SAMPLES, TXT, ATTN), 1.0, 6.0, ((0, 2), (1, 8)))
    image_query_gain = draw_image_query_gain(jax.random.fold_in(key_of[16], 71), part)
    image_key_gain = draw_image_key_gain(jax.random.fold_in(key_of[16], 71), part)
    text_query_gain = jnp.clip(jnp.exp(jax.random.uniform(key_of[8], (HEAD_DIM,), jnp.float32, math.log(1.2), math.log(2.5))), 1.2, 2.5)
    text_key_gain = jnp.clip(jnp.exp(jax.random.uniform(key_of[9], (HEAD_DIM,), jnp.float32, math.log(1.2), math.log(2.5))), 1.2, 2.5)
    text_length = jax.random.randint(own_keys[10], (SAMPLES,), 1, TXT + 1).astype(jnp.int32)
    strata = jax.random.randint(own_keys[11], (SAMPLES,), 0, STRATA).astype(jnp.int32)
    image_state = gaussian(own_keys[12], (SAMPLES, IMG, D), 1.0, 6.0, ((0, 2), (1, 8)))
    target = draw_target(jax.random.fold_in(jax.random.fold_in(key_of[16], part), 71), part)
    out_weight = gaussian(key_of[14], (ATTN, D), ATTN ** -0.5, 0.125, ((0, 4), (1, 2)))
    gate_table = gaussian(key_of[15], (STRATA, D), 1.0, 4.0)
    return dict(query_image=query_image, key_image=key_image, value_image=value_image, query_text=query_text, key_text=key_text, value_text=value_text, image_query_gain=image_query_gain, image_key_gain=image_key_gain, text_query_gain=text_query_gain, text_key_gain=text_key_gain, text_length=text_length, strata=strata, image_state=image_state, target=target, out_weight=out_weight, gate_table=gate_table)


def head_norm(values, gain_vector):
    columns = values.shape[-1]
    shaped = values.astype(jnp.float32).reshape(values.shape[:-1] + (columns // HEAD_DIM, HEAD_DIM))
    inverse = lax.rsqrt(lax.optimization_barrier(jnp.mean(shaped * shaped, axis=-1, keepdims=True)) + 1e-06)
    return (shaped * inverse * gain_vector).reshape(values.shape).astype(jnp.bfloat16)

def reference(query_image, key_image, value_image, query_text, key_text, value_text, image_query_gain, image_key_gain, text_query_gain, text_key_gain, text_length, strata, image_state, target, out_weight, gate_table):
    queries = jnp.concatenate([head_norm(query_text, text_query_gain), head_norm(query_image, image_query_gain)], axis=1)
    keys_joint = jnp.concatenate([head_norm(key_text, text_key_gain), head_norm(key_image, image_key_gain)], axis=1)
    values_joint = jnp.concatenate([value_text, value_image], axis=1)
    length = TXT + IMG
    positions = jnp.arange(length, dtype=jnp.int32)
    usable = (positions[None, :] >= TXT) | (positions[None, :] < text_length[:, None])

    def single_head(index):
        sample = index // HEADS
        head_start = index % HEADS * HEAD_DIM
        query_block = lax.dynamic_slice_in_dim(queries[sample], head_start, HEAD_DIM, 1)
        key_block = lax.dynamic_slice_in_dim(keys_joint[sample], head_start, HEAD_DIM, 1)
        value_block = lax.dynamic_slice_in_dim(values_joint[sample], head_start, HEAD_DIM, 1)
        scores = jnp.dot(query_block, key_block.T, preferred_element_type=jnp.float32) * HEAD_DIM ** (-0.5)
        scores = jnp.where(usable[sample][None, :], scores, -1e+30)
        row_max = lax.optimization_barrier(jnp.max(scores, axis=1, keepdims=True))
        powers = jnp.exp(scores - row_max)
        weights = (powers / lax.optimization_barrier(jnp.sum(powers, axis=1, keepdims=True))).astype(jnp.bfloat16)
        return jnp.dot(weights, value_block, preferred_element_type=jnp.float32).astype(jnp.bfloat16)
    heads_out = lax.map(single_head, jnp.arange(SAMPLES * HEADS, dtype=jnp.int32))
    attention = heads_out.reshape(SAMPLES, HEADS, length, HEAD_DIM).transpose(0, 2, 1, 3).reshape(SAMPLES, length, HEADS * HEAD_DIM)
    text_attention = attention[:, :TXT]
    image_rows = attention[:, TXT:].reshape(SAMPLES * IMG, HEADS * HEAD_DIM)
    branch = jnp.dot(image_rows, out_weight, preferred_element_type=jnp.float32).reshape(SAMPLES, IMG, D)
    gate_rows = gate_table[strata].astype(jnp.float32)
    combined = image_state.astype(jnp.float32) + gate_rows[:, None, :] * branch
    error_terms = combined - target.astype(jnp.float32)
    flow_loss = (jnp.sum(error_terms * error_terms) / (SAMPLES * IMG * D)).reshape(1)
    return (combined.astype(jnp.bfloat16), text_attention, flow_loss)
```

```python
import functools
import math

import jax
import jax.numpy as jnp
from jax import lax
from jax.experimental import pallas as pl
from jax.experimental.pallas import tpu as pltpu
from jax.sharding import PartitionSpec as P

VMEM = pltpu.MemorySpace.VMEM
SMEM = pltpu.MemorySpace.SMEM


def vmem_specs(count):
    return [pl.BlockSpec(memory_space=VMEM) for _ in range(count)]


def norm_rows(values, gain_row, head_dim):
    wide = values.astype(jnp.float32)
    inverse = lax.rsqrt(jnp.sum(wide * wide, axis=-1, keepdims=True) * (1.0 / head_dim) + 1e-06)
    return (wide * inverse * gain_row).astype(jnp.bfloat16)


def pack_kv_body(key_image, key_text, value_image, value_text, image_gain, text_gain, *outs, head_dim):
    count = len(outs)
    width = key_image.shape[1] // count
    text = key_text.shape[0]
    own = lax.axis_index("seq")
    for j, out in enumerate(outs):
        start = pl.multiple_of(lax.rem(own + j, count) * width, width)
        for h in range(width // head_dim):
            here = pl.ds(pl.multiple_of(start + h * head_dim, head_dim), head_dim)
            there = slice(h * head_dim, (h + 1) * head_dim)
            out[0, :text, there] = norm_rows(key_text[:, here], text_gain[...], head_dim)
            out[0, text:, there] = norm_rows(key_image[:, here], image_gain[...], head_dim)
        out[1, :text, :] = value_text[:, pl.ds(start, width)]
        out[1, text:, :] = value_image[:, pl.ds(start, width)]


def pack_q_body(query_image, query_text, image_gain, text_gain, *outs, head_dim):
    count = len(outs)
    width = query_image.shape[1] // count
    text = query_text.shape[0]
    own = lax.axis_index("seq")
    for j, out in enumerate(outs):
        start = pl.multiple_of(lax.rem(own + j, count) * width, width)
        for h in range(width // head_dim):
            here = pl.ds(pl.multiple_of(start + h * head_dim, head_dim), head_dim)
            there = slice(h * head_dim, (h + 1) * head_dim)
            out[:text, there] = norm_rows(query_text[:, here], text_gain[...], head_dim)
            out[text:, there] = norm_rows(query_image[:, here], image_gain[...], head_dim)


def attend_body(length, *refs, queries, pieces, cores, text, head_dim, kinds):
    query_refs = refs[:queries]
    kv_refs = refs[queries:queries + pieces]
    weight_refs = refs[queries + pieces:queries + pieces + cores]
    out_refs = refs[queries + pieces + cores:queries * 3 + pieces + cores]
    keys, values, heads_out = refs[queries * 3 + pieces + cores:]
    rows, width = query_refs[0].shape
    image = rows - text
    text_total = text * pieces
    ring = lax.axis_size("seq")
    own = lax.axis_index("seq")
    own_core = lax.axis_index("tp")
    for i, ref in enumerate(kv_refs):
        for target, plane in ((keys, 0), (values, 1)):
            target[i * text:(i + 1) * text, :] = ref[plane, :text, :]
            target[text_total + i * image:text_total + (i + 1) * image, :] = ref[plane, text:, :]
    lane = lax.broadcasted_iota(jnp.int32, (1, text_total), 1)
    position = lane
    for i in range(pieces):
        shard = lax.rem(own + ring - i // cores, ring)
        core = lax.rem(own_core + i % cores, cores)
        place = (shard * cores + core - i) * text
        inside = (lane >= i * text) & (lane < (i + 1) * text)
        position = jnp.where(inside, lane + place, position)
    usable = position < length[0]
    scale = head_dim ** (-0.5) * math.log2(math.e)
    for b, query in enumerate(query_refs):
        for h in range(width // head_dim):
            cols = slice(h * head_dim, (h + 1) * head_dim)
            raw = lax.dot_general(
                query[:, cols], keys[:, cols], (((1,), (1,)), ((), ())), preferred_element_type=jnp.float32
            )
            text_part = jnp.where(usable, raw[:, :text_total], -1e30)
            image_part = raw[:, text_total:]
            top = jnp.maximum(
                jnp.max(text_part, axis=1, keepdims=True), jnp.max(image_part, axis=1, keepdims=True)
            )
            text_power = jnp.exp2((text_part - top) * scale)
            image_power = jnp.exp2((image_part - top) * scale)
            total = jnp.sum(text_power, axis=1, keepdims=True) + jnp.sum(image_power, axis=1, keepdims=True)
            inverse = 1.0 / total
            weights = jnp.concatenate(
                [(text_power * inverse).astype(jnp.bfloat16), (image_power * inverse).astype(jnp.bfloat16)], axis=1
            )
            heads_out[:, cols] = jnp.dot(
                weights, values[:, cols], preferred_element_type=jnp.float32
            ).astype(jnp.bfloat16)
        out_refs[2 * b + 1][...] = heads_out[:text, :]
        half = weight_refs[0].shape[1]
        for c, weight in enumerate(weight_refs):
            start = pl.multiple_of(lax.rem(own_core + c, cores) * half, half)
            out_refs[2 * b][:, pl.ds(start, half)] = jnp.dot(
                heads_out[text:, :], weight[...], preferred_element_type=jnp.float32
            ).astype(kinds[b])


def finish_body(strata, own_part, *refs, arrivals, count):
    arrival_refs = refs[:arrivals]
    state, target, table = refs[arrivals:arrivals + 3]
    text_refs = refs[arrivals + 3:arrivals + 3 + count]
    velocity, text_out, loss = refs[arrivals + 3 + count:]
    own = lax.axis_index("seq")
    row = lax.broadcasted_iota(jnp.int32, table.shape, 0)
    gate = jnp.sum(jnp.where(row == strata[0], table[...].astype(jnp.float32), 0.0), axis=0, keepdims=True)
    branch = own_part[...]
    for ref in arrival_refs:
        branch = branch + ref[...].astype(jnp.float32)
    combined = state[...].astype(jnp.float32) + gate * branch
    velocity[...] = combined.astype(jnp.bfloat16)
    error = combined - target[...].astype(jnp.float32)
    loss[...] = jnp.sum(error * error).reshape(1, 1)
    width = text_out.shape[1] // count
    for j, ref in enumerate(text_refs):
        start = pl.multiple_of(lax.rem(own + count - j, count) * width, width)
        text_out[:, pl.ds(start, width)] = ref[...]


def shift(ring, amount):
    return [(i, (i + amount) % ring) for i in range(ring)]


def both_ways(ring, cores, amount):
    pairs = []
    for i in range(ring):
        for c in range(cores):
            step = amount if c % 2 == 0 else -amount
            pairs.append((i * cores + c, (i + step) % ring * cores + c))
    return pairs


def exchange(blocks, ring, cores):
    arrived = [None] * ring
    arrived[0] = blocks[0]
    middle = ring // 2 if ring % 2 == 0 else None
    if middle:
        halfway = blocks[middle]
        if middle > 1:
            halfway = lax.ppermute(halfway, ("seq", "tp"), both_ways(ring, cores, middle - 1))
    for j in range(1, (ring + 1) // 2):
        arrived[j] = lax.ppermute(blocks[j], "seq", shift(ring, j))
        arrived[ring - j] = lax.ppermute(blocks[ring - j], "seq", shift(ring, -j))
    if middle:
        arrived[middle] = lax.ppermute(halfway, ("seq", "tp"), both_ways(ring, cores, 1))
    return arrived


def all_sum(value, axes):
    for axis in axes:
        size = lax.axis_size(axis)
        if size & (size - 1):
            value = lax.psum(value, axis)
            continue
        step = 1
        while step < size:
            value = value + lax.ppermute(value, axis, [(i, i ^ step) for i in range(size)])
            step *= 2
    return value


def one_sample(
    query_image, key_image, value_image, query_text, key_text, value_text,
    gains, text_length, strata, image_state, target, weights, gate_table,
):
    image, columns = query_image.shape
    text = query_text.shape[0]
    rows = image + text
    model_width = gate_table.shape[1]
    head_dim = gains[0].shape[1]
    ring = lax.axis_size("seq")
    cores = lax.axis_size("tp")
    width = columns // ring
    bf16 = jnp.bfloat16
    kv_blocks = pl.pallas_call(
        functools.partial(pack_kv_body, head_dim=head_dim),
        out_shape=[jax.ShapeDtypeStruct((2, rows, width), bf16)] * ring,
        in_specs=vmem_specs(6),
        out_specs=vmem_specs(ring),
        name="pack_kv",
    )(key_image, key_text, value_image, value_text, gains[1], gains[3])
    kv_arrived = exchange(kv_blocks, ring, cores)
    q_blocks = pl.pallas_call(
        functools.partial(pack_q_body, head_dim=head_dim),
        out_shape=[jax.ShapeDtypeStruct((rows, width), bf16)] * ring,
        in_specs=vmem_specs(4),
        out_specs=vmem_specs(ring),
        name="pack_q",
    )(query_image, query_text, gains[0], gains[2])
    q_arrived = exchange(q_blocks, ring, cores)
    pieces = []
    for piece in kv_arrived:
        pieces.append(piece)
        for c in range(1, cores):
            pieces.append(lax.ppermute(piece, "tp", [((i + c) % cores, i) for i in range(cores)]))

    def attend(blocks, kinds, name):
        shapes = []
        for kind in kinds:
            shapes.append(jax.ShapeDtypeStruct((image, model_width), kind))
            shapes.append(jax.ShapeDtypeStruct((text, width), bf16))
        keys_shape = (rows * ring * cores, width)
        out = pl.pallas_call(
            functools.partial(
                attend_body, queries=len(blocks), pieces=len(pieces), cores=cores,
                text=text, head_dim=head_dim, kinds=kinds,
            ),
            out_shape=shapes,
            in_specs=[pl.BlockSpec(memory_space=SMEM)] + vmem_specs(len(blocks) + len(pieces) + cores),
            out_specs=vmem_specs(len(shapes)),
            scratch_shapes=[
                pltpu.VMEM(keys_shape, bf16), pltpu.VMEM(keys_shape, bf16), pltpu.VMEM((rows, width), bf16)
            ],
            name=name,
        )(text_length, *blocks, *pieces, *weights)
        return out[0::2], out[1::2]

    return attend, q_arrived


def local(
    query_image, key_image, value_image, query_text, key_text, value_text,
    image_query_gain, image_key_gain, text_query_gain, text_key_gain,
    text_length, strata, image_state, target, out_weight, gate_table,
):
    samples, image, _ = query_image.shape
    text = query_text.shape[1]
    model_width = gate_table.shape[1]
    ring = lax.axis_size("seq")
    cores = lax.axis_size("tp")
    up_count = ring // 2
    down_count = (ring - 1) // 2
    up_core = lax.axis_index("tp") % 2 == 0
    gains = [g.reshape(1, -1) for g in (image_query_gain, image_key_gain, text_query_gain, text_key_gain)]
    weights = [out_weight]
    for c in range(1, cores):
        weights.append(lax.ppermute(out_weight, "tp", [((i + c) % cores, i) for i in range(cores)]))
    velocities, texts, losses = [], [], []
    for s in range(samples):
        attend, q = one_sample(
            query_image[s], key_image[s], value_image[s], query_text[s], key_text[s], value_text[s],
            gains, text_length[s:s + 1], strata[s:s + 1], image_state[s], target[s], weights, gate_table,
        )
        parts = {}
        text_rows = {}
        first = [ring // 2] if ring % 2 == 0 else []
        rest = [j for j in range(ring) if j not in first]
        if first:
            (parts_first,), (text_first,) = attend([q[first[0]]], [jnp.bfloat16], "attend_far")
            parts[first[0]] = parts_first
            text_rows[first[0]] = text_first
        rest_parts, rest_text = attend(
            [q[j] for j in rest], [jnp.float32 if j == 0 else jnp.bfloat16 for j in rest], "attend_rest"
        )
        for j, part, t in zip(rest, rest_parts, rest_text):
            parts[j] = part
            text_rows[j] = t

        def toward(sign, j):
            up = parts[(ring - j) % ring]
            down = parts[j % ring]
            if up is down:
                return up
            pick_up = up_core if sign == 1 else jnp.logical_not(up_core)
            return jnp.where(pick_up, up, down)

        arrivals = []
        for sign, count in ((1, up_count), (-1, down_count)):
            carried = None
            for j in range(count, 0, -1):
                part = toward(sign, j)
                if carried is not None:
                    part = (part.astype(jnp.float32) + carried.astype(jnp.float32)).astype(jnp.bfloat16)
                carried = lax.ppermute(part, ("seq", "tp"), both_ways(ring, cores, sign))
            if carried is not None:
                arrivals.append(carried)
        text_arrived = [text_rows[0]] + [
            lax.ppermute(text_rows[j], "seq", shift(ring, -j)) for j in range(1, ring)
        ]
        text_down = [text_arrived[(ring - j) % ring] for j in range(ring)]
        velocity, text_out, loss = pl.pallas_call(
            functools.partial(finish_body, arrivals=len(arrivals), count=ring),
            out_shape=[
                jax.ShapeDtypeStruct((image, model_width), jnp.bfloat16),
                jax.ShapeDtypeStruct((text, query_image.shape[2]), jnp.bfloat16),
                jax.ShapeDtypeStruct((1, 1), jnp.float32),
            ],
            in_specs=[pl.BlockSpec(memory_space=SMEM)] + vmem_specs(1 + len(arrivals) + 3 + ring),
            out_specs=vmem_specs(3),
            name="finish",
        )(strata[s:s + 1], parts[0], *arrivals, image_state[s], target[s], gate_table, *text_down)
        velocities.append(velocity)
        texts.append(text_out)
        losses.append(loss)
    total = sum(losses[1:], losses[0])
    total = all_sum(total, ("tp", "dp", "seq"))
    element_count = samples * image * model_width * ring * cores * lax.axis_size("dp")
    flow_loss = (total / element_count).reshape(1)
    return jnp.stack(velocities), jnp.stack(texts), flow_loss


def solution(mesh):
    tokens = P(("grp", "dp"), ("seq", "tp"), None)
    placed = (tokens,) * 6 + (P(),) * 4 + (P(("grp", "dp")),) * 2 + (tokens,) * 2 + (P("seq", "tp"), P())
    return jax.shard_map(
        local, mesh=mesh, in_specs=placed, out_specs=(tokens, tokens, P("grp")), check_vma=False
    )
```
